32 devices in a mesh: dp: 1 (over z), sp: 32 (over x, y, core).
Axes of the slice: x: 4, y: 4, z: 1, core: 2. Of those that a mesh axis runs over, the one named last changes fastest.
The devices are a block of a 4x4x8 slice.
Arguments:
- q: bfloat16 [32, 56, 128], P('dp')
- k: bfloat16 [32, 4096, 56, 128], P('dp', 'sp')
- v: bfloat16 [32, 4096, 56, 128], P('dp', 'sp')
Outputs:
- q: bfloat16 [32, 56, 128], P('dp')
All inputs are finite; a program needn't handle non-finite values.
Results may differ from the reference program's by a relative error of at most 0.012.
Values are sent between devices in bfloat16 or wider.
A program may use at most 768 MiB of HBM per device.

```python
import jax
import jax.numpy as jnp

BATCH = 32
CACHE = 4096
HEADS = 56
KV_HEADS = 56
HEAD = 128


def setup_inputs(seed: int = 0, part: int = 0) -> dict:
    kq, kk, kv = (jax.random.fold_in(k, part) for k in jax.random.split(jax.random.key(seed), 3))
    return {
        "q": (3 * jax.random.normal(kq, (BATCH, HEADS, HEAD), jnp.float32)).astype(jnp.bfloat16),
        "k": jax.random.normal(kk, (BATCH, CACHE, KV_HEADS, HEAD), jnp.float32).astype(jnp.bfloat16),
        "v": jax.random.normal(kv, (BATCH, CACHE, KV_HEADS, HEAD), jnp.float32).astype(jnp.bfloat16),
    }


def einsum(form, a, b):
    return jnp.einsum(form, a.astype(jnp.float32), b.astype(jnp.float32))


def reference(q, k, v):
    grouped = q.reshape(BATCH, KV_HEADS, -1, HEAD)
    scores = einsum("bgsd,bugd->bgsu", grouped, k) * HEAD**-0.5
    weights = jax.nn.softmax(scores, -1).astype(jnp.bfloat16)
    return einsum("bgsu,bugd->bgsd", weights, v).astype(jnp.bfloat16).reshape(BATCH, HEADS, HEAD)
```

```python
import functools
import math

import jax
import jax.numpy as jnp
from jax import lax
from jax.experimental import pallas as pl
from jax.experimental.pallas import tpu as pltpu
from jax.sharding import PartitionSpec as P

MESH = pl.DeviceIdType.MESH
GROUP = 4
RING = 14
LAG = 5
TILE = 16
LANES = 256


def kernel(n, heads, scale, q_ref, k_ref, v_ref, out_ref, ring, qbuf, scores, pick, spread, stat, stats, high, share, parts, inbox, mine, ring_sem, q_sem, stat_send, stat_recv, part_send, part_recv, out_send, out_recv):
    me = lax.axis_index("sp")
    pairs, rows, head = k_ref.shape[0], k_ref.shape[2], k_ref.shape[3]
    width = pick.shape[1]
    chunks = rows // width
    both = 2 * heads
    per_pair = both // TILE
    blocks = pairs * per_pair

    def item(t):
        slot = lax.rem(t, RING)
        return ring.at[slot], ring_sem.at[slot]

    def fetch(t):
        dst, sem = item(t)

        @pl.when(t < pairs)
        def _():
            pltpu.make_async_copy(k_ref.at[t], dst, sem).start()

        @pl.when(jnp.logical_and(t >= pairs, t < 2 * pairs))
        def _():
            pltpu.make_async_copy(v_ref.at[t - pairs], dst, sem).start()

    def arrived(t):
        dst, sem = item(t)
        pltpu.make_async_copy(k_ref.at[0], dst, sem).wait()

    def peers(act):
        def one(s, _):
            act(lax.rem(me + s, n))
            return 0

        lax.fori_loop(1, n, one, 0)

    load_q = pltpu.make_async_copy(q_ref, qbuf, q_sem)
    load_q.start()
    for t in range(RING):
        fetch(jnp.int32(t))
    barrier = pltpu.get_barrier_semaphore()
    peers(lambda peer: pl.semaphore_signal(barrier, inc=1, device_id={"sp": peer}, device_id_type=MESH))

    column_head = lax.rem(lax.broadcasted_iota(jnp.int32, (TILE, width), 1), heads)
    row = lax.broadcasted_iota(jnp.int32, (TILE, width), 0)
    for r in range(0, heads, 8):
        pick[r : r + 8, :] = jnp.where(column_head[:8] == row[:8] + r, 1.0, 0.0)
    entries = [(i, b) for i in range(per_pair) for b in range(2) if i * TILE < (b + 1) * heads and (i + 1) * TILE > b * heads]
    for e, (i, b) in enumerate(entries):
        spread[e] = jnp.where(column_head == row + (i * TILE - b * heads), 1.0, 0.0).astype(jnp.bfloat16)
    stat[...] = jnp.zeros_like(stat)

    def fold(x, op):
        shift = width // 2
        while shift >= heads:
            x = op(x, pltpu.roll(x, shift, 1))
            shift //= 2
        return x

    def per_sequence(x, reduce):
        return [reduce(x[b * chunks : (b + 1) * chunks], 0, keepdims=True) for b in range(2)]

    def over_chunks(two):
        return jnp.concatenate([jnp.broadcast_to(x, (chunks, width)) for x in two], 0)

    def score(p):
        kv, _ = item(p)
        qp = qbuf[p].astype(jnp.float32)
        first = lax.broadcasted_iota(jnp.int32, (both, head), 0) < heads
        qq = jnp.concatenate([jnp.where(first, qp, 0.0), jnp.where(first, 0.0, qp)], 1).astype(jnp.bfloat16)
        for c in range(chunks):
            for j in range(width // LANES):
                at = pl.ds(c * width + j * LANES, LANES)
                cols = slice(j * LANES, (j + 1) * LANES)
                kk = jnp.concatenate([kv[0, at, :], kv[1, at, :]], 1)
                s = lax.dot_general(qq, kk, (((1,), (1,)), ((), ())), preferred_element_type=jnp.float32)
                wanted = pick[:, cols] != 0.0
                for b in range(2):
                    own = jnp.where(wanted, s[b * heads : (b + 1) * heads], 0.0)
                    scores[p, b * chunks + c : b * chunks + c + 1, cols] = jnp.sum(own, 0, keepdims=True)

    lane = lax.broadcasted_iota(jnp.int32, (1, 128), 1)
    tile_row = lax.broadcasted_iota(jnp.int32, (8, 128), 0)

    def local_stats(p):
        s = scores[p] * scale
        top = per_sequence(fold(s, jnp.maximum), jnp.max)
        total = per_sequence(fold(jnp.exp(s - over_chunks(top)), jnp.add), jnp.sum)
        at = lax.rem(p, GROUP)
        old = stat[...]
        for two, first in ((top, 0), (total, GROUP)):
            line = jnp.where(lane < heads, two[0][:, :128], two[1][:, :128])
            old = jnp.where(tile_row == at + first, jnp.broadcast_to(line, (8, 128)), old)
        stat[...] = old

    def send_stats(g):
        stats[g, me] = stat[...]
        peers(
            lambda peer: pltpu.make_async_remote_copy(
                stats.at[g, me], stats.at[g, me], stat_send.at[g], stat_recv.at[g], device_id={"sp": peer}, device_id_type=MESH
            ).start()
        )

    def all_stats(g):
        some = stats.at[g, pl.ds(0, n - 1)]
        pltpu.make_async_copy(some, some, stat_recv.at[g]).wait()
        x = stats[g]
        top = jnp.max(x, 0, keepdims=True)
        scaled = jnp.exp(pltpu.roll(x - top, GROUP, 1)) * x
        total = jnp.sum(scaled, 0)
        for ref, four in ((high, top[0, :GROUP]), (share, 1.0 / total[GROUP:])):
            lanes = lax.broadcasted_iota(jnp.int32, (GROUP, 128), 1)
            eight = jnp.concatenate([jnp.where(lanes < heads, four, 0.0), jnp.where(jnp.logical_and(lanes >= heads, lanes < both), four, 0.0)], 0)
            wide = jnp.concatenate([eight, jnp.zeros((2 * GROUP, width - 128), jnp.float32)], 1)
            shift = heads
            while shift < width:
                wide = wide + pltpu.roll(wide, shift, 1)
                shift *= 2
            for i in range(GROUP):
                ref[i] = over_chunks([wide[i : i + 1], wide[GROUP + i : GROUP + i + 1]])

    def attend(p):
        kv, _ = item(p + pairs)
        at = lax.rem(p, GROUP)
        w = jnp.exp(scores[p] * scale - high[at]) * share[at]
        acc = jnp.zeros((both, 2 * head), jnp.float32)
        for c in range(chunks):
            lines = [jnp.broadcast_to(w[b * chunks + c : b * chunks + c + 1], (TILE, width)).astype(jnp.bfloat16) for b in range(2)]
            lhs = [None] * per_pair
            for e, (i, b) in enumerate(entries):
                term = lines[b] * spread[e]
                lhs[i] = term if lhs[i] is None else lhs[i] + term
            vv = jnp.concatenate([kv[0, c * width : (c + 1) * width, :], kv[1, c * width : (c + 1) * width, :]], 1)
            acc = acc + jnp.dot(jnp.concatenate(lhs, 0), vv, preferred_element_type=jnp.float32)
        part = jnp.concatenate([acc[:heads, :head], acc[heads:, head:]], 0).astype(jnp.bfloat16)
        for i in range(per_pair):
            parts[p * per_pair + i] = part[i * TILE : (i + 1) * TILE]

    def part_copy(b):
        return pltpu.make_async_remote_copy(
            parts.at[b], inbox.at[b // n, me], part_send.at[b], part_recv.at[b // n], device_id={"sp": lax.rem(b, n)}, device_id_type=MESH
        )

    def send_parts(p):
        def one(i, _):
            b = p * per_pair + i

            @pl.when(lax.rem(b, n) == me)
            def _():
                inbox[b // n, me] = parts[b]

            @pl.when(lax.rem(b, n) != me)
            def _():
                part_copy(b).start()

            return 0

        lax.fori_loop(0, per_pair, one, 0)

    def add_up(p):
        i = lax.rem(me + n * blocks - p * per_pair, n)

        @pl.when(i < per_pair)
        def _():
            b = p * per_pair + i
            j = b // n
            some = inbox.at[j, pl.ds(0, n - 1)]
            pltpu.make_async_copy(some, some, part_recv.at[j]).wait()
            mine[j] = jnp.sum(inbox[j].astype(jnp.float32), 0).astype(jnp.bfloat16)
            pltpu.make_async_copy(mine.at[j], out_ref.at[b], out_recv).start()
            peers(
                lambda peer: pltpu.make_async_remote_copy(
                    mine.at[j], out_ref.at[b], out_send.at[j], out_recv, device_id={"sp": peer}, device_id_type=MESH
                ).start()
            )

    load_q.wait()
    arrived(jnp.int32(0))
    score(0)
    fetch(jnp.int32(RING))
    pl.semaphore_wait(barrier, n - 1)

    def key_step(p, _):
        arrived(p)
        local_stats(p - 1)
        score(p)
        fetch(p + RING)

        @pl.when(lax.rem(p, GROUP) == 0)
        def _():
            send_stats(p // GROUP - 1)

        return 0

    lax.fori_loop(1, pairs, key_step, 0)
    local_stats(pairs - 1)
    send_stats(pairs // GROUP - 1)

    def value_step(p, _):
        @pl.when(lax.rem(p, GROUP) == 0)
        def _():
            all_stats(p // GROUP)

        arrived(p + pairs)
        attend(p)
        fetch(p + pairs + RING)
        send_parts(p)

        @pl.when(p >= LAG)
        def _():
            add_up(p - LAG)

        return 0

    lax.fori_loop(0, pairs, value_step, 0)

    def drain(p, _):
        add_up(p)
        return 0

    lax.fori_loop(pairs - LAG, pairs, drain, 0)

    for g in range(pairs // GROUP):
        some = stats.at[g, pl.ds(0, n - 1)]
        pltpu.make_async_copy(some, some, stat_send.at[g]).wait()

    def sent(b, _):
        @pl.when(lax.rem(b, n) != me)
        def _():
            part_copy(b).wait_send()

        return 0

    lax.fori_loop(0, blocks, sent, 0)
    for j in range(mine.shape[0]):

        @pl.when(j * n + me < blocks)
        def _():
            some = inbox.at[j, pl.ds(0, n - 1)]
            pltpu.make_async_copy(some, some, out_send.at[j]).wait()

    pltpu.make_async_copy(out_ref, out_ref, out_recv).wait()


def solution(mesh):
    n = mesh.shape["sp"]

    def step(q, k, v):
        batch, heads, head = q.shape
        tokens = k.shape[1]
        pairs, rows = batch // 2, tokens * heads
        width = math.lcm(heads, LANES)
        chunks = rows // width
        per_pair = 2 * heads // TILE
        blocks = pairs * per_pair
        owned = -(-blocks // n)
        groups = pairs // GROUP
        entries = per_pair + (heads % TILE != 0)
        f32, bf16 = jnp.float32, jnp.bfloat16
        out = pl.pallas_call(
            functools.partial(kernel, n, heads, head**-0.5),
            out_shape=jax.ShapeDtypeStruct((blocks, TILE, head), bf16),
            in_specs=[pl.BlockSpec(memory_space=pl.ANY)] * 3,
            out_specs=pl.BlockSpec(memory_space=pl.ANY),
            scratch_shapes=[
                pltpu.VMEM((RING, 2, rows, head), bf16),
                pltpu.VMEM((pairs, 2 * heads, head), bf16),
                pltpu.VMEM((pairs, 2 * chunks, width), f32),
                pltpu.VMEM((heads, width), f32),
                pltpu.VMEM((entries, TILE, width), bf16),
                pltpu.VMEM((2 * GROUP, 128), f32),
                pltpu.VMEM((groups, n, 2 * GROUP, 128), f32),
                pltpu.VMEM((GROUP, 2 * chunks, width), f32),
                pltpu.VMEM((GROUP, 2 * chunks, width), f32),
                pltpu.VMEM((blocks, TILE, head), bf16),
                pltpu.VMEM((owned, n, TILE, head), bf16),
                pltpu.VMEM((owned, TILE, head), bf16),
                pltpu.SemaphoreType.DMA((RING,)),
                pltpu.SemaphoreType.DMA,
                pltpu.SemaphoreType.DMA((groups,)),
                pltpu.SemaphoreType.DMA((groups,)),
                pltpu.SemaphoreType.DMA((blocks,)),
                pltpu.SemaphoreType.DMA((owned,)),
                pltpu.SemaphoreType.DMA((owned,)),
                pltpu.SemaphoreType.DMA,
            ],
            compiler_params=pltpu.CompilerParams(collective_id=0, has_side_effects=True, vmem_limit_bytes=66 * 1000 * 1000),
            cost_estimate=pl.CostEstimate(flops=8 * batch * rows * head, bytes_accessed=4 * batch * rows * head, transcendentals=2 * batch * rows),
            name="attend",
        )(q.reshape(pairs, 2 * heads, head), k.reshape(pairs, 2, rows, head), v.reshape(pairs, 2, rows, head))
        return out.reshape(q.shape)

    return jax.shard_map(
        step,
        mesh=mesh,
        in_specs=(P("dp", None, None), P("dp", "sp", None, None), P("dp", "sp", None, None)),
        out_specs=P("dp", None, None),
        check_vma=False,
    )
```

```python
import functools

import jax
import jax.numpy as jnp
from jax import lax
from jax.experimental import pallas as pl
from jax.experimental.pallas import tpu as pltpu
from jax.sharding import PartitionSpec as P

MESH = pl.DeviceIdType.MESH
GROUP = 8
RING = 6
AHEAD = 3
LAG = 6
TILE = 16
SUB = 8
LANES = 128


def kernel(n, heads, scale, q_ref, k_ref, v_ref, out_ref, ring, qbuf, scores, spread, stat, stats, high, share, parts, inbox, mine, ring_sem, q_sem, stat_send, stat_recv, part_send, part_recv, out_send, out_recv):
    me = lax.axis_index("sp")
    pairs, rows, head = k_ref.shape[0], k_ref.shape[2], k_ref.shape[3]
    both = 2 * heads
    per_pair = both // TILE
    blocks = pairs * per_pair
    slabs = heads // SUB
    twos = rows // both // SUB
    span = rows // SUB

    def wrap(x):
        return jnp.where(x >= n, x - n, x)

    def item(t):
        slot = lax.rem(t, RING)
        return ring.at[slot], ring_sem.at[slot]

    def fetch(t):
        dst, sem = item(t)

        @pl.when(t < pairs)
        def _():
            pltpu.make_async_copy(k_ref.at[t], dst, sem).start()

        @pl.when(jnp.logical_and(t >= pairs, t < 2 * pairs))
        def _():
            pltpu.make_async_copy(v_ref.at[t - pairs], dst, sem).start()

    def arrived(t):
        dst, sem = item(t)
        pltpu.make_async_copy(k_ref.at[0], dst, sem).wait()

    def peers(act):
        for s in range(1, n):
            act(wrap(me + s))

    load_q = pltpu.make_async_copy(q_ref, qbuf, q_sem)
    load_q.start()
    for t in range(AHEAD):
        fetch(jnp.int32(t))
    barrier = pltpu.get_barrier_semaphore()
    peers(lambda peer: pl.semaphore_signal(barrier, inc=1, device_id={"sp": peer}, device_id_type=MESH))

    column_head = lax.rem(lax.broadcasted_iota(jnp.int32, (TILE, span), 1), heads)
    row = lax.broadcasted_iota(jnp.int32, (TILE, span), 0)
    entries = [(i, b) for i in range(per_pair) for b in range(2) if i * TILE < (b + 1) * heads and (i + 1) * TILE > b * heads]
    for e, (i, b) in enumerate(entries):
        spread[e] = jnp.where(column_head == row + (i * TILE - b * heads), 1.0, 0.0).astype(jnp.bfloat16)
    stat[...] = jnp.zeros_like(stat)

    lane = lax.broadcasted_iota(jnp.int32, (SUB, LANES), 1)
    sub = lax.broadcasted_iota(jnp.int32, (SUB, LANES), 0)
    own = [jnp.logical_or(lane == sub + i * SUB, lane == sub + (i * SUB + heads)) for i in range(slabs)]

    def score(p):
        kv, _ = item(p)
        qp = jnp.concatenate([qbuf[p].astype(jnp.float32), jnp.zeros((LANES - both, head), jnp.float32)], 0)
        first = lax.broadcasted_iota(jnp.int32, (LANES, head), 0) < heads
        qq = jnp.concatenate([jnp.where(first, qp, 0.0), jnp.where(first, 0.0, qp)], 1).astype(jnp.bfloat16)
        for r in range(twos):
            at = [slice((s * twos + r) * both, (s * twos + r + 1) * both) for s in range(SUB)]
            kk = jnp.concatenate([jnp.concatenate([kv[0, a, :], kv[1, a, :]], 1) for a in at], 0)
            x = lax.dot_general(kk, qq, (((1,), (1,)), ((), ())), preferred_element_type=jnp.float32)
            x = x.reshape(2 * SUB, slabs, SUB, LANES)
            y = jnp.where(own[0], x[:, 0], 0.0)
            for i in range(1, slabs):
                y = jnp.where(own[i], x[:, i], y)
            y = y.reshape(SUB, 2, SUB, LANES)
            for k in (4, 2, 1):
                low, high_ = y[:k], y[k:]
                y = jnp.where(lax.rem(sub // k, 2) == 0, low + pltpu.roll(low, SUB - k, 2), high_ + pltpu.roll(high_, k, 2))
            for e in range(2):
                scores[p, e, r] = y[0, e]

    stat_row = lax.broadcasted_iota(jnp.int32, (GROUP, LANES), 0)

    def local_stats(p):
        s = scores[p] * scale
        top = jnp.max(jnp.max(s, (0, 1)), 0, keepdims=True)
        total = jnp.sum(jnp.sum(jnp.exp(s - top), (0, 1)), 0, keepdims=True)
        at = stat_row == lax.rem(p, GROUP)
        stat[0] = jnp.where(at, top, stat[0])
        stat[1] = jnp.where(at, total, stat[1])

    def send_stats(g):
        stats[g, me] = stat[...]
        peers(
            lambda peer: pltpu.make_async_remote_copy(
                stats.at[g, me], stats.at[g, me], stat_send.at[g], stat_recv.at[g], device_id={"sp": peer}, device_id_type=MESH
            ).start()
        )

    def all_stats(g):
        some = stats.at[g, pl.ds(0, n - 1)]
        pltpu.make_async_copy(some, some, stat_recv.at[g]).wait()
        tops, totals = stats[g, :, 0], stats[g, :, 1]
        top = jnp.max(tops, 0)
        inverse = 1.0 / jnp.sum(totals * jnp.exp(tops - top), 0)
        for i in range(GROUP):
            high[i] = jnp.broadcast_to(top[i : i + 1], (SUB, LANES))
            share[i] = jnp.broadcast_to(inverse[i : i + 1], (SUB, LANES))

    def attend(p):
        kv, _ = item(p + pairs)
        at = lax.rem(p, GROUP)
        even, odd = jnp.exp(scores[p] * scale - high[at]) * share[at]
        left = lane < heads
        flat = []
        for two in (jnp.where(left, even, pltpu.roll(odd, heads, 2)), jnp.where(left, pltpu.roll(even, LANES - heads, 2), odd)):
            gap = LANES - both
            turned = [two[0]] + [pltpu.roll(two[r], LANES - gap * r, 1) for r in range(1, twos)]
            flat.append([jnp.where(lane < both - gap * c, turned[c], turned[c + 1]) for c in range(twos - 1)])
        flat = [jnp.concatenate(f, 1) for f in flat]
        acc = jnp.zeros((both, 2 * head), jnp.float32)
        for c in range(SUB // 2):
            lhs = []
            for s in (2 * c, 2 * c + 1):
                lines = [jnp.broadcast_to(flat[b][s : s + 1], (TILE, span)).astype(jnp.bfloat16) for b in range(2)]
                some = [None] * per_pair
                for e, (i, b) in enumerate(entries):
                    term = lines[b] * spread[e]
                    some[i] = term if some[i] is None else some[i] + term
                lhs.append(jnp.concatenate(some, 0))
            a = slice(2 * c * span, (2 * c + 2) * span)
            vv = jnp.concatenate([kv[0, a, :], kv[1, a, :]], 1)
            acc = acc + jnp.dot(jnp.concatenate(lhs, 1), vv, preferred_element_type=jnp.float32)
        part = jnp.concatenate([acc[:heads, :head], acc[heads:, head:]], 0).astype(jnp.bfloat16)
        for i in range(per_pair):
            parts[p * per_pair + i] = part[i * TILE : (i + 1) * TILE]

    def send_parts(p):
        base = p * per_pair
        round_, start = base // n, lax.rem(base, n)
        for i in range(per_pair):
            owner = wrap(start + i)

            @pl.when(owner != me)
            def _():
                pltpu.make_async_remote_copy(
                    parts.at[base + i],
                    inbox.at[jnp.where(start + i >= n, round_ + 1, round_), me],
                    part_send,
                    part_recv.at[jnp.where(start + i >= n, round_ + 1, round_)],
                    device_id={"sp": owner},
                    device_id_type=MESH,
                ).start()

    def add_up(p):
        i = lax.rem(me + n * blocks - p * per_pair, n)

        @pl.when(i < per_pair)
        def _():
            b = p * per_pair + i
            j = b // n
            inbox[j, me] = parts[b]
            some = inbox.at[j, pl.ds(0, n - 1)]
            with jax.named_scope("part_wait"):
                pltpu.make_async_copy(some, some, part_recv.at[j]).wait()
            mine[j] = jnp.sum(inbox[j].astype(jnp.float32), 0).astype(jnp.bfloat16)
            pltpu.make_async_copy(mine.at[j], out_ref.at[b], out_recv).start()
            peers(
                lambda peer: pltpu.make_async_remote_copy(
                    mine.at[j], out_ref.at[b], out_send.at[j], out_recv, device_id={"sp": peer}, device_id_type=MESH
                ).start()
            )

    with jax.named_scope("first_wait"):
        load_q.wait()
        arrived(jnp.int32(0))
    with jax.named_scope("first_keys"):
        fetch(jnp.int32(AHEAD))
        score(0)
    pl.semaphore_wait(barrier, n - 1)

    def key_step(p, _):
        with jax.named_scope("key_wait"):
            arrived(p)
        with jax.named_scope("keys"):
            fetch(p + AHEAD)
            local_stats(p - 1)
            score(p)

        @pl.when(lax.rem(p, GROUP) == 0)
        def _():
            with jax.named_scope("send_stats"):
                send_stats(p // GROUP - 1)

        return 0

    lax.fori_loop(1, pairs, key_step, 0)
    local_stats(pairs - 1)
    send_stats(pairs // GROUP - 1)

    def value_step(p, _):
        @pl.when(lax.rem(p, GROUP) == 0)
        def _():
            with jax.named_scope("all_stats"):
                all_stats(p // GROUP)

        with jax.named_scope("value_wait"):
            arrived(p + pairs)
        with jax.named_scope("values"):
            fetch(p + pairs + AHEAD)
            attend(p)
        with jax.named_scope("send_parts"):
            send_parts(p)

        @pl.when(p >= LAG)
        def _():
            add_up(p - LAG)

        return 0

    lax.fori_loop(0, pairs, value_step, 0)

    def drain(p, _):
        add_up(p)
        return 0

    with jax.named_scope("drain"):
        lax.fori_loop(pairs - LAG, pairs, drain, 0)

    for g in range(pairs // GROUP):
        some = stats.at[g, pl.ds(0, n - 1)]
        pltpu.make_async_copy(some, some, stat_send.at[g]).wait()
    for owned in {blocks // n, -(-blocks // n)}:

        @pl.when((me < blocks % n) == (owned > blocks // n))
        def _():
            some = parts.at[pl.ds(0, blocks - owned)]
            pltpu.make_async_copy(some, some, part_send).wait()

    for j in range(mine.shape[0]):

        @pl.when(j * n + me < blocks)
        def _():
            some = inbox.at[j, pl.ds(0, n - 1)]
            pltpu.make_async_copy(some, some, out_send.at[j]).wait()

    with jax.named_scope("last_wait"):
        pltpu.make_async_copy(out_ref, out_ref, out_recv).wait()


def solution(mesh):
    n = mesh.shape["sp"]

    def step(q, k, v):
        batch, heads, head = q.shape
        tokens = k.shape[1]
        pairs, rows = batch // 2, tokens * heads
        per_pair = 2 * heads // TILE
        blocks = pairs * per_pair
        owned = -(-blocks // n)
        groups = pairs // GROUP
        entries = per_pair + (heads % TILE != 0)
        f32, bf16 = jnp.float32, jnp.bfloat16
        out = pl.pallas_call(
            functools.partial(kernel, n, heads, head**-0.5),
            out_shape=jax.ShapeDtypeStruct((blocks, TILE, head), bf16),
            in_specs=[pl.BlockSpec(memory_space=pl.ANY)] * 3,
            out_specs=pl.BlockSpec(memory_space=pl.ANY),
            scratch_shapes=[
                pltpu.VMEM((RING, 2, rows, head), bf16),
                pltpu.VMEM((pairs, 2 * heads, head), bf16),
                pltpu.VMEM((pairs, 2, tokens // (2 * SUB), SUB, LANES), f32),
                pltpu.VMEM((entries, TILE, rows // SUB), bf16),
                pltpu.VMEM((2, GROUP, LANES), f32),
                pltpu.VMEM((groups, n, 2, GROUP, LANES), f32),
                pltpu.VMEM((GROUP, SUB, LANES), f32),
                pltpu.VMEM((GROUP, SUB, LANES), f32),
                pltpu.VMEM((blocks, TILE, head), bf16),
                pltpu.VMEM((owned, n, TILE, head), bf16),
                pltpu.VMEM((owned, TILE, head), bf16),
                pltpu.SemaphoreType.DMA((RING,)),
                pltpu.SemaphoreType.DMA,
                pltpu.SemaphoreType.DMA((groups,)),
                pltpu.SemaphoreType.DMA((groups,)),
                pltpu.SemaphoreType.DMA,
                pltpu.SemaphoreType.DMA((owned,)),
                pltpu.SemaphoreType.DMA((owned,)),
                pltpu.SemaphoreType.DMA,
            ],
            compiler_params=pltpu.CompilerParams(collective_id=0, has_side_effects=True, vmem_limit_bytes=40 * 1024 * 1024),
            cost_estimate=pl.CostEstimate(flops=8 * batch * rows * head, bytes_accessed=4 * batch * rows * head, transcendentals=2 * batch * rows),
            name="attend",
        )(q.reshape(pairs, 2 * heads, head), k.reshape(pairs, 2, rows, head), v.reshape(pairs, 2, rows, head))
        return out.reshape(q.shape)

    return jax.shard_map(
        step,
        mesh=mesh,
        in_specs=(P("dp", None, None), P("dp", "sp", None, None), P("dp", "sp", None, None)),
        out_specs=P("dp", None, None),
        check_vma=False,
    )
```

```python
import functools

import jax
import jax.numpy as jnp
from jax import lax
from jax.experimental import pallas as pl
from jax.experimental.pallas import tpu as pltpu
from jax.sharding import PartitionSpec as P

MESH = pl.DeviceIdType.MESH
GROUP = 8
RING = 6
AHEAD = 3
LAG = 6
TILE = 16
SUB = 8
LANES = 128


def kernel(n, heads, scale, q_ref, k_ref, v_ref, out_ref, ring, qbuf, scores, spread, stat, stats, high, share, parts, inbox, mine, ring_sem, q_sem, stat_send, stat_recv, part_send, part_recv, out_send, out_recv):
    me = lax.axis_index("sp")
    pairs, rows, head = k_ref.shape[0], k_ref.shape[2], k_ref.shape[3]
    both = 2 * heads
    per_pair = both // TILE
    blocks = pairs * per_pair
    slabs = heads // SUB
    twos = rows // both // SUB
    span = rows // SUB
    stride = 5 if n % 5 else 1

    def wrap(x):
        return jnp.where(x >= n, x - n, x)

    def item(t):
        slot = lax.rem(t, RING)
        return ring.at[slot], ring_sem.at[slot]

    def fetch(t):
        dst, sem = item(t)

        @pl.when(t < pairs)
        def _():
            pltpu.make_async_copy(k_ref.at[t], dst, sem).start()

        @pl.when(jnp.logical_and(t >= pairs, t < 2 * pairs))
        def _():
            pltpu.make_async_copy(v_ref.at[t - pairs], dst, sem).start()

    def arrived(t):
        dst, sem = item(t)
        pltpu.make_async_copy(k_ref.at[0], dst, sem).wait()

    def peers(act):
        for s in range(1, n):
            act(wrap(me + s))

    load_q = pltpu.make_async_copy(q_ref, qbuf, q_sem)
    load_q.start()
    for t in range(AHEAD):
        fetch(jnp.int32(t))
    barrier = pltpu.get_barrier_semaphore()
    peers(lambda peer: pl.semaphore_signal(barrier, inc=1, device_id={"sp": peer}, device_id_type=MESH))

    column_head = lax.rem(lax.broadcasted_iota(jnp.int32, (TILE, span), 1), heads)
    row = lax.broadcasted_iota(jnp.int32, (TILE, span), 0)
    entries = [(i, b) for i in range(per_pair) for b in range(2) if i * TILE < (b + 1) * heads and (i + 1) * TILE > b * heads]
    for e, (i, b) in enumerate(entries):
        spread[e] = jnp.where(column_head == row + (i * TILE - b * heads), 1.0, 0.0).astype(jnp.bfloat16)
    stat[...] = jnp.zeros_like(stat)

    lane = lax.broadcasted_iota(jnp.int32, (SUB, LANES), 1)
    sub = lax.broadcasted_iota(jnp.int32, (SUB, LANES), 0)
    own = [jnp.logical_or(lane == sub + i * SUB, lane == sub + (i * SUB + heads)) for i in range(slabs)]

    def score(p):
        kv, _ = item(p)
        qp = jnp.concatenate([qbuf[p].astype(jnp.float32), jnp.zeros((LANES - both, head), jnp.float32)], 0)
        first = lax.broadcasted_iota(jnp.int32, (LANES, head), 0) < heads
        qq = jnp.concatenate([jnp.where(first, qp, 0.0), jnp.where(first, 0.0, qp)], 1).astype(jnp.bfloat16)
        for r in range(twos):
            at = [slice((s * twos + r) * both, (s * twos + r + 1) * both) for s in range(SUB)]
            kk = jnp.concatenate([jnp.concatenate([kv[0, a, :], kv[1, a, :]], 1) for a in at], 0)
            x = lax.dot_general(kk, qq, (((1,), (1,)), ((), ())), preferred_element_type=jnp.float32)
            x = x.reshape(2 * SUB, slabs, SUB, LANES)
            y = jnp.where(own[0], x[:, 0], 0.0)
            for i in range(1, slabs):
                y = jnp.where(own[i], x[:, i], y)
            y = y.reshape(SUB, 2, SUB, LANES)
            for k in (4, 2, 1):
                low, high_ = y[:k], y[k:]
                y = jnp.where(lax.rem(sub // k, 2) == 0, low + pltpu.roll(low, SUB - k, 2), high_ + pltpu.roll(high_, k, 2))
            for e in range(2):
                scores[p, e, r] = y[0, e]

    stat_row = lax.broadcasted_iota(jnp.int32, (GROUP, LANES), 0)

    def local_stats(p):
        s = scores[p] * scale
        top = jnp.max(jnp.max(s, (0, 1)), 0, keepdims=True)
        total = jnp.sum(jnp.sum(jnp.exp(s - top), (0, 1)), 0, keepdims=True)
        at = stat_row == lax.rem(p, GROUP)
        stat[0] = jnp.where(at, top, stat[0])
        stat[1] = jnp.where(at, total, stat[1])

    def send_stats(g):
        stats[g, me] = stat[...]
        peers(
            lambda peer: pltpu.make_async_remote_copy(
                stats.at[g, me], stats.at[g, me], stat_send.at[g], stat_recv.at[g], device_id={"sp": peer}, device_id_type=MESH
            ).start()
        )

    def all_stats(g):
        some = stats.at[g, pl.ds(0, n - 1)]
        pltpu.make_async_copy(some, some, stat_recv.at[g]).wait()
        tops, totals = stats[g, :, 0], stats[g, :, 1]
        top = jnp.max(tops, 0)
        inverse = 1.0 / jnp.sum(totals * jnp.exp(tops - top), 0)
        for i in range(GROUP):
            high[i] = jnp.broadcast_to(top[i : i + 1], (SUB, LANES))
            share[i] = jnp.broadcast_to(inverse[i : i + 1], (SUB, LANES))

    def attend(p):
        kv, _ = item(p + pairs)
        at = lax.rem(p, GROUP)
        even, odd = jnp.exp(scores[p] * scale - high[at]) * share[at]
        left = lane < heads
        flat = []
        for two in (jnp.where(left, even, pltpu.roll(odd, heads, 2)), jnp.where(left, pltpu.roll(even, LANES - heads, 2), odd)):
            gap = LANES - both
            turned = [two[0]] + [pltpu.roll(two[r], LANES - gap * r, 1) for r in range(1, twos)]
            flat.append([jnp.where(lane < both - gap * c, turned[c], turned[c + 1]) for c in range(twos - 1)])
        flat = [jnp.concatenate(f, 1) for f in flat]
        acc = [jnp.zeros((both, 2 * head), jnp.float32)] * 2
        for c in range(SUB // 2):
            lhs = []
            for s in (2 * c, 2 * c + 1):
                lines = [jnp.broadcast_to(flat[b][s : s + 1], (TILE, span)).astype(jnp.bfloat16) for b in range(2)]
                some = [None] * per_pair
                for e, (i, b) in enumerate(entries):
                    term = lines[b] * spread[e]
                    some[i] = term if some[i] is None else some[i] + term
                lhs.append(jnp.concatenate(some, 0))
            a = slice(2 * c * span, (2 * c + 2) * span)
            vv = jnp.concatenate([kv[0, a, :], kv[1, a, :]], 1)
            acc[c % 2] = acc[c % 2] + jnp.dot(jnp.concatenate(lhs, 1), vv, preferred_element_type=jnp.float32)
        acc = acc[0] + acc[1]
        part = jnp.concatenate([acc[:heads, :head], acc[heads:, head:]], 0).astype(jnp.bfloat16)
        for i in range(per_pair):
            parts[p * per_pair + i] = part[i * TILE : (i + 1) * TILE]

    def send_parts(p):
        for i in range(per_pair):
            b = p * per_pair + i
            owner = lax.rem(b * stride, n)

            @pl.when(owner != me)
            def _():
                pltpu.make_async_remote_copy(
                    parts.at[b], inbox.at[lax.div(b, n), me], part_send, part_recv.at[lax.div(b, n)], device_id={"sp": owner}, device_id_type=MESH
                ).start()

    def add_up(p):
        i = lax.rem(me * pow(stride, -1, n) + n * blocks - p * per_pair, n)

        @pl.when(i < per_pair)
        def _():
            b = p * per_pair + i
            j = lax.div(b, n)
            inbox[j, me] = parts[b]
            some = inbox.at[j, pl.ds(0, n - 1)]
            with jax.named_scope("part_wait"):
                pltpu.make_async_copy(some, some, part_recv.at[j]).wait()
            mine[j] = jnp.sum(inbox[j].astype(jnp.float32), 0).astype(jnp.bfloat16)
            pltpu.make_async_copy(mine.at[j], out_ref.at[b], out_recv).start()
            peers(
                lambda peer: pltpu.make_async_remote_copy(
                    mine.at[j], out_ref.at[b], out_send.at[j], out_recv, device_id={"sp": peer}, device_id_type=MESH
                ).start()
            )

    with jax.named_scope("first_wait"):
        load_q.wait()
        arrived(jnp.int32(0))
    with jax.named_scope("first_keys"):
        score(0)
        arrived(jnp.int32(1))
        fetch(jnp.int32(AHEAD))
        fetch(jnp.int32(AHEAD + 1))
        score(1)
    pl.semaphore_wait(barrier, n - 1)

    def key_step(u, _):
        p = 2 * u
        with jax.named_scope("key_wait"):
            arrived(p)
            arrived(p + 1)
        with jax.named_scope("keys"):
            fetch(p + AHEAD)
            fetch(p + 1 + AHEAD)
            local_stats(p - 2)
            local_stats(p - 1)
            score(p)
            score(p + 1)

        @pl.when(lax.rem(p, GROUP) == 0)
        def _():
            with jax.named_scope("send_stats"):
                send_stats(lax.div(p, GROUP) - 1)

        return 0

    lax.fori_loop(1, pairs // 2, key_step, 0)
    local_stats(pairs - 2)
    local_stats(pairs - 1)
    send_stats(pairs // GROUP - 1)

    def value_step(u, _):
        p = 2 * u

        @pl.when(lax.rem(p, GROUP) == 0)
        def _():
            with jax.named_scope("all_stats"):
                all_stats(lax.div(p, GROUP))

        with jax.named_scope("value_wait"):
            arrived(p + pairs)
            arrived(p + 1 + pairs)
        with jax.named_scope("values"):
            fetch(p + pairs + AHEAD)
            fetch(p + 1 + pairs + AHEAD)
            attend(p)
            attend(p + 1)
        with jax.named_scope("send_parts"):
            send_parts(p)
            send_parts(p + 1)

        @pl.when(p >= LAG)
        def _():
            add_up(p - LAG)
            add_up(p + 1 - LAG)

        return 0

    lax.fori_loop(0, pairs // 2 - 1, value_step, 0)
    for p in (pairs - 2, pairs - 1):
        with jax.named_scope("value_wait"):
            arrived(jnp.int32(p + pairs))
        with jax.named_scope("values"):
            attend(jnp.int32(p))
        with jax.named_scope("send_parts"):
            send_parts(jnp.int32(p))

    def drain(p, _):
        add_up(p)
        return 0

    with jax.named_scope("drain"):
        lax.fori_loop(pairs - LAG - 2, pairs, drain, 0)

    for g in range(pairs // GROUP):
        some = stats.at[g, pl.ds(0, n - 1)]
        pltpu.make_async_copy(some, some, stat_send.at[g]).wait()
    for owned in {blocks // n, -(-blocks // n)}:

        @pl.when((lax.rem(me * pow(stride, -1, n), n) < blocks % n) == (owned > blocks // n))
        def _():
            some = parts.at[pl.ds(0, blocks - owned)]
            pltpu.make_async_copy(some, some, part_send).wait()

    for j in range(mine.shape[0]):

        @pl.when(j * n + lax.rem(me * pow(stride, -1, n), n) < blocks)
        def _():
            some = inbox.at[j, pl.ds(0, n - 1)]
            pltpu.make_async_copy(some, some, out_send.at[j]).wait()

    with jax.named_scope("last_wait"):
        pltpu.make_async_copy(out_ref, out_ref, out_recv).wait()


def solution(mesh):
    n = mesh.shape["sp"]

    def step(q, k, v):
        batch, heads, head = q.shape
        tokens = k.shape[1]
        pairs, rows = batch // 2, tokens * heads
        per_pair = 2 * heads // TILE
        blocks = pairs * per_pair
        owned = -(-blocks // n)
        groups = pairs // GROUP
        entries = per_pair + (heads % TILE != 0)
        f32, bf16 = jnp.float32, jnp.bfloat16
        out = pl.pallas_call(
            functools.partial(kernel, n, heads, head**-0.5),
            out_shape=jax.ShapeDtypeStruct((blocks, TILE, head), bf16),
            in_specs=[pl.BlockSpec(memory_space=pl.ANY)] * 3,
            out_specs=pl.BlockSpec(memory_space=pl.ANY),
            scratch_shapes=[
                pltpu.VMEM((RING, 2, rows, head), bf16),
                pltpu.VMEM((pairs, 2 * heads, head), bf16),
                pltpu.VMEM((pairs, 2, tokens // (2 * SUB), SUB, LANES), f32),
                pltpu.VMEM((entries, TILE, rows // SUB), bf16),
                pltpu.VMEM((2, GROUP, LANES), f32),
                pltpu.VMEM((groups, n, 2, GROUP, LANES), f32),
                pltpu.VMEM((GROUP, SUB, LANES), f32),
                pltpu.VMEM((GROUP, SUB, LANES), f32),
                pltpu.VMEM((blocks, TILE, head), bf16),
                pltpu.VMEM((owned, n, TILE, head), bf16),
                pltpu.VMEM((owned, TILE, head), bf16),
                pltpu.SemaphoreType.DMA((RING,)),
                pltpu.SemaphoreType.DMA,
                pltpu.SemaphoreType.DMA((groups,)),
                pltpu.SemaphoreType.DMA((groups,)),
                pltpu.SemaphoreType.DMA,
                pltpu.SemaphoreType.DMA((owned,)),
                pltpu.SemaphoreType.DMA((owned,)),
                pltpu.SemaphoreType.DMA,
            ],
            compiler_params=pltpu.CompilerParams(collective_id=0, has_side_effects=True, vmem_limit_bytes=53 * 1024 * 1024 + 400 * 1024),
            cost_estimate=pl.CostEstimate(flops=8 * batch * rows * head, bytes_accessed=4 * batch * rows * head, transcendentals=2 * batch * rows),
            name="attend",
        )(q.reshape(pairs, 2 * heads, head), k.reshape(pairs, 2, rows, head), v.reshape(pairs, 2, rows, head))
        return out.reshape(q.shape)

    return jax.shard_map(
        step,
        mesh=mesh,
        in_specs=(P("dp", None, None), P("dp", "sp", None, None), P("dp", "sp", None, None)),
        out_specs=P("dp", None, None),
        check_vma=False,
    )
```

```python
import functools

import jax
import jax.numpy as jnp
from jax import lax
from jax.experimental import pallas as pl
from jax.experimental.pallas import tpu as pltpu
from jax.sharding import PartitionSpec as P

MESH = pl.DeviceIdType.MESH
GROUP = 8
RING = 7
AHEAD = 5
FIRST = 4
LAG = 6
TILE = 16
SUB = 8
LANES = 128


def kernel(n, heads, scale, q_ref, k_ref, v_ref, out_ref, ring, qbuf, scores, spread, stat, stats, high, share, parts, inbox, mine, ring_sem, q_sem, stat_send, stat_recv, part_send, part_recv, out_send, out_recv):
    me = lax.axis_index("sp")
    pairs, rows, head = k_ref.shape[0], k_ref.shape[2], k_ref.shape[3]
    both = 2 * heads
    per_pair = both // TILE
    blocks = pairs * per_pair
    slabs = heads // SUB
    twos = rows // both // SUB
    span = rows // SUB
    stride = 5 if n % 5 else 1

    def wrap(x):
        return jnp.where(x >= n, x - n, x)

    def item(t):
        slot = lax.rem(t, RING)
        return ring.at[slot], ring_sem.at[slot]

    def fetch(t):
        dst, sem = item(t)

        @pl.when(t < pairs)
        def _():
            pltpu.make_async_copy(k_ref.at[t], dst, sem).start()

        @pl.when(jnp.logical_and(t >= pairs, t < 2 * pairs))
        def _():
            pltpu.make_async_copy(v_ref.at[t - pairs], dst, sem).start()

    def arrived(t):
        dst, sem = item(t)
        pltpu.make_async_copy(k_ref.at[0], dst, sem).wait()

    def peers(act):
        for s in sorted(range(1, n), key=lambda s: abs(s - n * 5 // 8)):
            act(wrap(me + s))

    load_q = pltpu.make_async_copy(q_ref, qbuf, q_sem)
    load_q.start()
    for t in range(FIRST):
        fetch(jnp.int32(t))
    barrier = pltpu.get_barrier_semaphore()
    peers(lambda peer: pl.semaphore_signal(barrier, inc=1, device_id={"sp": peer}, device_id_type=MESH))

    column_head = lax.rem(lax.broadcasted_iota(jnp.int32, (TILE, span), 1), heads)
    row = lax.broadcasted_iota(jnp.int32, (TILE, span), 0)
    entries = [(i, b) for i in range(per_pair) for b in range(2) if i * TILE < (b + 1) * heads and (i + 1) * TILE > b * heads]
    for e, (i, b) in enumerate(entries):
        spread[e] = jnp.where(column_head == row + (i * TILE - b * heads), 1.0, 0.0).astype(jnp.bfloat16)
    stat[...] = jnp.zeros_like(stat)

    lane = lax.broadcasted_iota(jnp.int32, (SUB, LANES), 1)
    sub = lax.broadcasted_iota(jnp.int32, (SUB, LANES), 0)
    own = [jnp.logical_or(lane == sub + i * SUB, lane == sub + (i * SUB + heads)) for i in range(slabs)]

    def score(p):
        kv, _ = item(p)
        qp = jnp.concatenate([qbuf[p].astype(jnp.float32), jnp.zeros((LANES - both, head), jnp.float32)], 0)
        first = lax.broadcasted_iota(jnp.int32, (LANES, head), 0) < heads
        qq = jnp.concatenate([jnp.where(first, qp, 0.0), jnp.where(first, 0.0, qp)], 1).astype(jnp.bfloat16)
        for r in range(twos):
            at = [slice((s * twos + r) * both, (s * twos + r + 1) * both) for s in range(SUB)]
            kk = jnp.concatenate([jnp.concatenate([kv[0, a, :], kv[1, a, :]], 1) for a in at], 0)
            x = lax.dot_general(kk, qq, (((1,), (1,)), ((), ())), preferred_element_type=jnp.float32)
            x = x.reshape(2 * SUB, slabs, SUB, LANES)
            y = jnp.where(own[0], x[:, 0], 0.0)
            for i in range(1, slabs):
                y = jnp.where(own[i], x[:, i], y)
            y = y.reshape(SUB, 2, SUB, LANES)
            for k in (4, 2, 1):
                low, high_ = y[:k], y[k:]
                y = jnp.where(lax.rem(sub // k, 2) == 0, low + pltpu.roll(low, SUB - k, 2), high_ + pltpu.roll(high_, k, 2))
            for e in range(2):
                scores[p, e, r] = y[0, e]

    stat_row = lax.broadcasted_iota(jnp.int32, (GROUP, LANES), 0)

    def local_stats(p):
        s = scores[p] * scale
        top = jnp.max(jnp.max(s, (0, 1)), 0, keepdims=True)
        total = jnp.sum(jnp.sum(jnp.exp(s - top), (0, 1)), 0, keepdims=True)
        at = stat_row == lax.rem(p, GROUP)
        stat[0] = jnp.where(at, top, stat[0])
        stat[1] = jnp.where(at, total, stat[1])

    def send_stats(g):
        stats[g, me] = stat[...]
        peers(
            lambda peer: pltpu.make_async_remote_copy(
                stats.at[g, me], stats.at[g, me], stat_send.at[g], stat_recv.at[g], device_id={"sp": peer}, device_id_type=MESH
            ).start()
        )

    def all_stats(g):
        some = stats.at[g, pl.ds(0, n - 1)]
        pltpu.make_async_copy(some, some, stat_recv.at[g]).wait()
        tops, totals = stats[g, :, 0], stats[g, :, 1]
        top = jnp.max(tops, 0)
        inverse = 1.0 / jnp.sum(totals * jnp.exp(tops - top), 0)
        for i in range(GROUP):
            high[i] = jnp.broadcast_to(top[i : i + 1], (SUB, LANES))
            share[i] = jnp.broadcast_to(inverse[i : i + 1], (SUB, LANES))

    def attend(p):
        kv, _ = item(p + pairs)
        at = lax.rem(p, GROUP)
        even, odd = jnp.exp(scores[p] * scale - high[at]) * share[at]
        left = lane < heads
        flat = []
        for two in (jnp.where(left, even, pltpu.roll(odd, heads, 2)), jnp.where(left, pltpu.roll(even, LANES - heads, 2), odd)):
            gap = LANES - both
            turned = [two[0]] + [pltpu.roll(two[r], LANES - gap * r, 1) for r in range(1, twos)]
            flat.append([jnp.where(lane < both - gap * c, turned[c], turned[c + 1]) for c in range(twos - 1)])
        flat = [jnp.concatenate(f, 1) for f in flat]
        acc = [jnp.zeros((both, 2 * head), jnp.float32)] * 2
        for c in range(SUB // 2):
            lhs = []
            for s in (2 * c, 2 * c + 1):
                lines = [jnp.broadcast_to(flat[b][s : s + 1], (TILE, span)).astype(jnp.bfloat16) for b in range(2)]
                some = [None] * per_pair
                for e, (i, b) in enumerate(entries):
                    term = lines[b] * spread[e]
                    some[i] = term if some[i] is None else some[i] + term
                lhs.append(jnp.concatenate(some, 0))
            a = slice(2 * c * span, (2 * c + 2) * span)
            vv = jnp.concatenate([kv[0, a, :], kv[1, a, :]], 1)
            acc[c % 2] = acc[c % 2] + jnp.dot(jnp.concatenate(lhs, 1), vv, preferred_element_type=jnp.float32)
        acc = acc[0] + acc[1]
        part = jnp.concatenate([acc[:heads, :head], acc[heads:, head:]], 0).astype(jnp.bfloat16)
        for i in range(per_pair):
            parts[p * per_pair + i] = part[i * TILE : (i + 1) * TILE]

    def send_parts(p):
        for i in range(per_pair):
            b = p * per_pair + i
            owner = lax.rem(b * stride, n)

            @pl.when(owner != me)
            def _():
                pltpu.make_async_remote_copy(
                    parts.at[b], inbox.at[lax.div(b, n), me], part_send, part_recv.at[lax.div(b, n)], device_id={"sp": owner}, device_id_type=MESH
                ).start()

    def add_up(p):
        i = lax.rem(me * pow(stride, -1, n) + n * blocks - p * per_pair, n)

        @pl.when(i < per_pair)
        def _():
            b = p * per_pair + i
            j = lax.div(b, n)
            inbox[j, me] = parts[b]
            some = inbox.at[j, pl.ds(0, n - 1)]
            with jax.named_scope("part_wait"):
                pltpu.make_async_copy(some, some, part_recv.at[j]).wait()
            mine[j] = jnp.sum(inbox[j].astype(jnp.float32), 0).astype(jnp.bfloat16)
            pltpu.make_async_copy(mine.at[j], out_ref.at[b], out_recv).start()
            peers(
                lambda peer: pltpu.make_async_remote_copy(
                    mine.at[j], out_ref.at[b], out_send.at[j], out_recv, device_id={"sp": peer}, device_id_type=MESH
                ).start()
            )

    with jax.named_scope("first_wait"):
        load_q.wait()
        arrived(jnp.int32(0))
    with jax.named_scope("first_keys"):
        fetch(jnp.int32(FIRST))
        score(0)
        arrived(jnp.int32(1))
        for t in range(FIRST + 1, AHEAD + 2):
            fetch(jnp.int32(t))
        score(1)
    pl.semaphore_wait(barrier, n - 1)

    def key_step(u, _):
        p = 2 * u
        with jax.named_scope("key_wait"):
            arrived(p)
            arrived(p + 1)
        with jax.named_scope("keys"):
            fetch(p + AHEAD)
            fetch(p + 1 + AHEAD)
            local_stats(p - 2)
            local_stats(p - 1)
            score(p)
            score(p + 1)

        @pl.when(lax.rem(p, GROUP) == 0)
        def _():
            with jax.named_scope("send_stats"):
                send_stats(lax.div(p, GROUP) - 1)

        return 0

    lax.fori_loop(1, pairs // 2, key_step, 0)
    local_stats(pairs - 2)
    local_stats(pairs - 1)
    send_stats(pairs // GROUP - 1)

    def value_step(u, _):
        p = 2 * u

        @pl.when(lax.rem(p, GROUP) == 0)
        def _():
            with jax.named_scope("all_stats"):
                all_stats(lax.div(p, GROUP))

        with jax.named_scope("value_wait"):
            arrived(p + pairs)
            arrived(p + 1 + pairs)
        with jax.named_scope("values"):
            fetch(p + pairs + AHEAD)
            fetch(p + 1 + pairs + AHEAD)
            attend(p)
            attend(p + 1)
        with jax.named_scope("send_parts"):
            send_parts(p)
            send_parts(p + 1)

        @pl.when(p >= LAG)
        def _():
            add_up(p - LAG)
            add_up(p + 1 - LAG)

        return 0

    lax.fori_loop(0, pairs // 2, value_step, 0)

    def drain(p, _):
        add_up(p)
        return 0

    with jax.named_scope("drain"):
        lax.fori_loop(pairs - LAG, pairs, drain, 0)

    for g in range(pairs // GROUP):
        some = stats.at[g, pl.ds(0, n - 1)]
        pltpu.make_async_copy(some, some, stat_send.at[g]).wait()
    for owned in {blocks // n, -(-blocks // n)}:

        @pl.when((lax.rem(me * pow(stride, -1, n), n) < blocks % n) == (owned > blocks // n))
        def _():
            some = parts.at[pl.ds(0, blocks - owned)]
            pltpu.make_async_copy(some, some, part_send).wait()

    for j in range(mine.shape[0]):

        @pl.when(j * n + lax.rem(me * pow(stride, -1, n), n) < blocks)
        def _():
            some = inbox.at[j, pl.ds(0, n - 1)]
            pltpu.make_async_copy(some, some, out_send.at[j]).wait()

    with jax.named_scope("last_wait"):
        pltpu.make_async_copy(out_ref, out_ref, out_recv).wait()


def solution(mesh):
    n = mesh.shape["sp"]

    def step(q, k, v):
        batch, heads, head = q.shape
        tokens = k.shape[1]
        pairs, rows = batch // 2, tokens * heads
        per_pair = 2 * heads // TILE
        blocks = pairs * per_pair
        owned = -(-blocks // n)
        groups = pairs // GROUP
        entries = per_pair + (heads % TILE != 0)
        f32, bf16 = jnp.float32, jnp.bfloat16
        out = pl.pallas_call(
            functools.partial(kernel, n, heads, head**-0.5),
            out_shape=jax.ShapeDtypeStruct((blocks, TILE, head), bf16),
            in_specs=[pl.BlockSpec(memory_space=pl.ANY)] * 3,
            out_specs=pl.BlockSpec(memory_space=pl.ANY),
            scratch_shapes=[
                pltpu.VMEM((RING, 2, rows, head), bf16),
                pltpu.VMEM((pairs, 2 * heads, head), bf16),
                pltpu.VMEM((pairs, 2, tokens // (2 * SUB), SUB, LANES), f32),
                pltpu.VMEM((entries, TILE, rows // SUB), bf16),
                pltpu.VMEM((2, GROUP, LANES), f32),
                pltpu.VMEM((groups, n, 2, GROUP, LANES), f32),
                pltpu.VMEM((GROUP, SUB, LANES), f32),
                pltpu.VMEM((GROUP, SUB, LANES), f32),
                pltpu.VMEM((blocks, TILE, head), bf16),
                pltpu.VMEM((owned, n, TILE, head), bf16),
                pltpu.VMEM((owned, TILE, head), bf16),
                pltpu.SemaphoreType.DMA((RING,)),
                pltpu.SemaphoreType.DMA,
                pltpu.SemaphoreType.DMA((groups,)),
                pltpu.SemaphoreType.DMA((groups,)),
                pltpu.SemaphoreType.DMA,
                pltpu.SemaphoreType.DMA((owned,)),
                pltpu.SemaphoreType.DMA((owned,)),
                pltpu.SemaphoreType.DMA,
            ],
            compiler_params=pltpu.CompilerParams(collective_id=0, has_side_effects=True, vmem_limit_bytes=53 * 1024 * 1024 + 400 * 1024),
            cost_estimate=pl.CostEstimate(flops=8 * batch * rows * head, bytes_accessed=4 * batch * rows * head, transcendentals=2 * batch * rows),
            name="attend",
        )(q.reshape(pairs, 2 * heads, head), k.reshape(pairs, 2, rows, head), v.reshape(pairs, 2, rows, head))
        return out.reshape(q.shape)

    return jax.shard_map(
        step,
        mesh=mesh,
        in_specs=(P("dp", None, None), P("dp", "sp", None, None), P("dp", "sp", None, None)),
        out_specs=P("dp", None, None),
        check_vma=False,
    )
```

```python
import functools

import jax
import jax.numpy as jnp
from jax import lax
from jax.experimental import pallas as pl
from jax.experimental.pallas import tpu as pltpu
from jax.sharding import PartitionSpec as P

MESH = pl.DeviceIdType.MESH
GROUP = 8
RING = 6
AHEAD = 4
FIRST = 3
LAG = 6
TILE = 16
SUB = 8
LANES = 128


def kernel(n, heads, scale, q_ref, k_ref, v_ref, out_ref, ring, qbuf, scores, spread, stat, stats, high, share, parts, inbox, mine, ring_sem, q_sem, stat_send, stat_recv, part_send, part_recv, out_send, out_recv):
    me = lax.axis_index("sp")
    pairs, rows, head = k_ref.shape[0], k_ref.shape[2], k_ref.shape[3]
    both = 2 * heads
    per_pair = both // TILE
    blocks = pairs * per_pair
    slabs = heads // SUB
    twos = rows // both // SUB
    span = rows // SUB
    stride = 5 if n % 5 else 1

    def wrap(x):
        return jnp.where(x >= n, x - n, x)

    def item(t):
        slot = lax.rem(t, RING)
        return ring.at[slot], ring_sem.at[slot]

    def fetch(t):
        dst, sem = item(t)

        @pl.when(t < pairs)
        def _():
            pltpu.make_async_copy(k_ref.at[t], dst, sem).start()

        @pl.when(jnp.logical_and(t >= pairs, t < 2 * pairs))
        def _():
            pltpu.make_async_copy(v_ref.at[t - pairs], dst, sem).start()

    def arrived(t):
        dst, sem = item(t)
        pltpu.make_async_copy(k_ref.at[0], dst, sem).wait()

    def peers(act):
        for s in sorted(range(1, n), key=lambda s: abs(s - n * 5 // 8)):
            act(wrap(me + s))

    load_q = pltpu.make_async_copy(q_ref, qbuf, q_sem)
    load_q.start()
    fetch(jnp.int32(0))
    barrier = pltpu.get_barrier_semaphore()
    peers(lambda peer: pl.semaphore_signal(barrier, inc=1, device_id={"sp": peer}, device_id_type=MESH))

    fetch(jnp.int32(1))
    column_head = lax.rem(lax.broadcasted_iota(jnp.int32, (TILE, span), 1), heads)
    row = lax.broadcasted_iota(jnp.int32, (TILE, span), 0)
    entries = [(i, b) for i in range(per_pair) for b in range(2) if i * TILE < (b + 1) * heads and (i + 1) * TILE > b * heads]
    for e, (i, b) in enumerate(entries):
        spread[e] = jnp.where(column_head == row + (i * TILE - b * heads), 1.0, 0.0).astype(jnp.bfloat16)
    stat[...] = jnp.zeros_like(stat)
    for t in range(2, FIRST):
        fetch(jnp.int32(t))

    lane = lax.broadcasted_iota(jnp.int32, (SUB, LANES), 1)
    sub = lax.broadcasted_iota(jnp.int32, (SUB, LANES), 0)
    own = [jnp.logical_or(lane == sub + i * SUB, lane == sub + (i * SUB + heads)) for i in range(slabs)]

    def score(p):
        kv, _ = item(p)
        qp = jnp.concatenate([qbuf[p].astype(jnp.float32), jnp.zeros((LANES - both, head), jnp.float32)], 0)
        first = lax.broadcasted_iota(jnp.int32, (LANES, head), 0) < heads
        qq = jnp.concatenate([jnp.where(first, qp, 0.0), jnp.where(first, 0.0, qp)], 1).astype(jnp.bfloat16)
        for r in range(twos):
            at = [slice((s * twos + r) * both, (s * twos + r + 1) * both) for s in range(SUB)]
            kk = jnp.concatenate([jnp.concatenate([kv[0, a, :], kv[1, a, :]], 1) for a in at], 0)
            x = lax.dot_general(kk, qq, (((1,), (1,)), ((), ())), preferred_element_type=jnp.float32)
            x = x.reshape(2 * SUB, slabs, SUB, LANES)
            y = jnp.where(own[0], x[:, 0], 0.0)
            for i in range(1, slabs):
                y = jnp.where(own[i], x[:, i], y)
            y = y.reshape(SUB, 2, SUB, LANES)
            for k in (4, 2, 1):
                low, high_ = y[:k], y[k:]
                y = jnp.where(lax.rem(sub // k, 2) == 0, low + pltpu.roll(low, SUB - k, 2), high_ + pltpu.roll(high_, k, 2))
            for e in range(2):
                scores[p, e, r] = y[0, e]

    stat_row = lax.broadcasted_iota(jnp.int32, (GROUP, LANES), 0)

    def local_stats(p):
        s = scores[p] * scale
        top = jnp.max(jnp.max(s, (0, 1)), 0, keepdims=True)
        total = jnp.sum(jnp.sum(jnp.exp(s - top), (0, 1)), 0, keepdims=True)
        at = stat_row == lax.rem(p, GROUP)
        stat[0] = jnp.where(at, top, stat[0])
        stat[1] = jnp.where(at, total, stat[1])

    def send_stats(g):
        stats[g, me] = stat[...]
        peers(
            lambda peer: pltpu.make_async_remote_copy(
                stats.at[g, me], stats.at[g, me], stat_send.at[g], stat_recv.at[g], device_id={"sp": peer}, device_id_type=MESH
            ).start()
        )

    def all_stats(g):
        some = stats.at[g, pl.ds(0, n - 1)]
        pltpu.make_async_copy(some, some, stat_recv.at[g]).wait()
        tops, totals = stats[g, :, 0], stats[g, :, 1]
        top = jnp.max(tops, 0)
        inverse = 1.0 / jnp.sum(totals * jnp.exp(tops - top), 0)
        for i in range(GROUP):
            high[i] = jnp.broadcast_to(top[i : i + 1], (SUB, LANES))
            share[i] = jnp.broadcast_to(inverse[i : i + 1], (SUB, LANES))

    def attend(p):
        kv, _ = item(p + pairs)
        at = lax.rem(p, GROUP)
        even, odd = jnp.exp(scores[p] * scale - high[at]) * share[at]
        left = lane < heads
        flat = []
        for two in (jnp.where(left, even, pltpu.roll(odd, heads, 2)), jnp.where(left, pltpu.roll(even, LANES - heads, 2), odd)):
            gap = LANES - both
            turned = [two[0]] + [pltpu.roll(two[r], LANES - gap * r, 1) for r in range(1, twos)]
            flat.append([jnp.where(lane < both - gap * c, turned[c], turned[c + 1]) for c in range(twos - 1)])
        flat = [jnp.concatenate(f, 1) for f in flat]
        acc = [jnp.zeros((both, 2 * head), jnp.float32)] * 2
        for c in range(SUB // 2):
            lhs = []
            for s in (2 * c, 2 * c + 1):
                lines = [jnp.broadcast_to(flat[b][s : s + 1], (TILE, span)).astype(jnp.bfloat16) for b in range(2)]
                some = [None] * per_pair
                for e, (i, b) in enumerate(entries):
                    term = lines[b] * spread[e]
                    some[i] = term if some[i] is None else some[i] + term
                lhs.append(jnp.concatenate(some, 0))
            a = slice(2 * c * span, (2 * c + 2) * span)
            vv = jnp.concatenate([kv[0, a, :], kv[1, a, :]], 1)
            acc[c % 2] = acc[c % 2] + jnp.dot(jnp.concatenate(lhs, 1), vv, preferred_element_type=jnp.float32)
        acc = acc[0] + acc[1]
        part = jnp.concatenate([acc[:heads, :head], acc[heads:, head:]], 0).astype(jnp.bfloat16)
        for i in range(per_pair):
            parts[p * per_pair + i] = part[i * TILE : (i + 1) * TILE]

    def send_parts(p):
        for i in range(per_pair):
            b = p * per_pair + i
            owner = lax.rem(b * stride, n)

            @pl.when(owner != me)
            def _():
                pltpu.make_async_remote_copy(
                    parts.at[b], inbox.at[lax.div(b, n), me], part_send, part_recv.at[lax.div(b, n)], device_id={"sp": owner}, device_id_type=MESH
                ).start()

    def add_up(p):
        i = lax.rem(me * pow(stride, -1, n) + n * blocks - p * per_pair, n)

        @pl.when(i < per_pair)
        def _():
            b = p * per_pair + i
            j = lax.div(b, n)
            inbox[j, me] = parts[b]
            some = inbox.at[j, pl.ds(0, n - 1)]
            with jax.named_scope("part_wait"):
                pltpu.make_async_copy(some, some, part_recv.at[j]).wait()
            mine[j] = jnp.sum(inbox[j].astype(jnp.float32), 0).astype(jnp.bfloat16)
            pltpu.make_async_copy(mine.at[j], out_ref.at[b], out_recv).start()
            peers(
                lambda peer: pltpu.make_async_remote_copy(
                    mine.at[j], out_ref.at[b], out_send.at[j], out_recv, device_id={"sp": peer}, device_id_type=MESH
                ).start()
            )

    with jax.named_scope("first_wait"):
        load_q.wait()
        arrived(jnp.int32(0))
    with jax.named_scope("first_keys"):
        fetch(jnp.int32(FIRST))
        score(0)
        arrived(jnp.int32(1))
        for t in range(FIRST + 1, AHEAD + 2):
            fetch(jnp.int32(t))
        score(1)
    pl.semaphore_wait(barrier, n - 1)

    def key_step(u, _):
        p = 2 * u
        with jax.named_scope("key_wait"):
            arrived(p)
            arrived(p + 1)
        with jax.named_scope("keys"):
            fetch(p + AHEAD)
            fetch(p + 1 + AHEAD)
            local_stats(p - 2)
            local_stats(p - 1)
            score(p)
            score(p + 1)

        @pl.when(lax.rem(p, GROUP) == 0)
        def _():
            with jax.named_scope("send_stats"):
                send_stats(lax.div(p, GROUP) - 1)

        return 0

    lax.fori_loop(1, pairs // 2, key_step, 0)
    local_stats(pairs - 2)
    local_stats(pairs - 1)
    send_stats(pairs // GROUP - 1)

    def value_step(u, _):
        p = 2 * u

        @pl.when(lax.rem(p, GROUP) == 0)
        def _():
            with jax.named_scope("all_stats"):
                all_stats(lax.div(p, GROUP))

        with jax.named_scope("value_wait"):
            arrived(p + pairs)
            arrived(p + 1 + pairs)
        with jax.named_scope("values"):
            fetch(p + pairs + AHEAD)
            fetch(p + 1 + pairs + AHEAD)
            attend(p)
            attend(p + 1)
        with jax.named_scope("send_parts"):
            send_parts(p)
            send_parts(p + 1)

        @pl.when(p >= LAG)
        def _():
            add_up(p - LAG)
            add_up(p + 1 - LAG)

        return 0

    def single_step(p, _):
        with jax.named_scope("value_wait"):
            arrived(p + pairs)
        with jax.named_scope("values"):
            attend(p)
        with jax.named_scope("send_parts"):
            send_parts(p)
        return 0

    lax.fori_loop(0, pairs // 2 - 1, value_step, 0)
    lax.fori_loop(pairs - 2, pairs, single_step, 0)

    def drain(p, _):
        add_up(p)
        return 0

    with jax.named_scope("drain"):
        lax.fori_loop(pairs - LAG - 2, pairs, drain, 0)

    for g in range(pairs // GROUP):
        some = stats.at[g, pl.ds(0, n - 1)]
        pltpu.make_async_copy(some, some, stat_send.at[g]).wait()
    for owned in {blocks // n, -(-blocks // n)}:

        @pl.when((lax.rem(me * pow(stride, -1, n), n) < blocks % n) == (owned > blocks // n))
        def _():
            some = parts.at[pl.ds(0, blocks - owned)]
            pltpu.make_async_copy(some, some, part_send).wait()

    for j in range(mine.shape[0]):

        @pl.when(j * n + lax.rem(me * pow(stride, -1, n), n) < blocks)
        def _():
            some = inbox.at[j, pl.ds(0, n - 1)]
            pltpu.make_async_copy(some, some, out_send.at[j]).wait()

    with jax.named_scope("last_wait"):
        pltpu.make_async_copy(out_ref, out_ref, out_recv).wait()


def solution(mesh):
    n = mesh.shape["sp"]

    def step(q, k, v):
        batch, heads, head = q.shape
        tokens = k.shape[1]
        pairs, rows = batch // 2, tokens * heads
        per_pair = 2 * heads // TILE
        blocks = pairs * per_pair
        owned = -(-blocks // n)
        groups = pairs // GROUP
        entries = per_pair + (heads % TILE != 0)
        f32, bf16 = jnp.float32, jnp.bfloat16
        out = pl.pallas_call(
            functools.partial(kernel, n, heads, head**-0.5),
            out_shape=jax.ShapeDtypeStruct((blocks, TILE, head), bf16),
            in_specs=[pl.BlockSpec(memory_space=pl.ANY)] * 3,
            out_specs=pl.BlockSpec(memory_space=pl.ANY),
            scratch_shapes=[
                pltpu.VMEM((RING, 2, rows, head), bf16),
                pltpu.VMEM((pairs, 2 * heads, head), bf16),
                pltpu.VMEM((pairs, 2, tokens // (2 * SUB), SUB, LANES), f32),
                pltpu.VMEM((entries, TILE, rows // SUB), bf16),
                pltpu.VMEM((2, GROUP, LANES), f32),
                pltpu.VMEM((groups, n, 2, GROUP, LANES), f32),
                pltpu.VMEM((GROUP, SUB, LANES), f32),
                pltpu.VMEM((GROUP, SUB, LANES), f32),
                pltpu.VMEM((blocks, TILE, head), bf16),
                pltpu.VMEM((owned, n, TILE, head), bf16),
                pltpu.VMEM((owned, TILE, head), bf16),
                pltpu.SemaphoreType.DMA((RING,)),
                pltpu.SemaphoreType.DMA,
                pltpu.SemaphoreType.DMA((groups,)),
                pltpu.SemaphoreType.DMA((groups,)),
                pltpu.SemaphoreType.DMA,
                pltpu.SemaphoreType.DMA((owned,)),
                pltpu.SemaphoreType.DMA((owned,)),
                pltpu.SemaphoreType.DMA,
            ],
            compiler_params=pltpu.CompilerParams(collective_id=0, has_side_effects=True, vmem_limit_bytes=53 * 1024 * 1024 + 400 * 1024),
            cost_estimate=pl.CostEstimate(flops=8 * batch * rows * head, bytes_accessed=4 * batch * rows * head, transcendentals=2 * batch * rows),
            name="attend",
        )(q.reshape(pairs, 2 * heads, head), k.reshape(pairs, 2, rows, head), v.reshape(pairs, 2, rows, head))
        return out.reshape(q.shape)

    return jax.shard_map(
        step,
        mesh=mesh,
        in_specs=(P("dp", None, None), P("dp", "sp", None, None), P("dp", "sp", None, None)),
        out_specs=P("dp", None, None),
        check_vma=False,
    )
```
